512 devices in a mesh: groups: 2 (over y), expert: 32 (over z), tensor: 8 (over x, core).
Axes of the slice: x: 4, y: 2, z: 32, core: 2. Of those that a mesh axis runs over, the one named last changes fastest.
The devices are a block of a 4x8x32 slice.
Arguments:
- tokens: bfloat16 [8192, 7168], P(('groups', 'expert'), 'tensor'), parts along dimension 0, may hold values from -6 to 6
- choices: int32 [8192, 4], P(('groups', 'expert')), parts along dimension 0, may hold values from 0 to 15, all different within a row; in each aligned block of 128 rows (0 to 127, 128 to 255, ...) at most 48 rows name the same one
- affinity: float32 [8192, 4], P(('groups', 'expert')), parts along dimension 0, may hold values from -6 to 6
- expert_gate: bfloat16 [7168, 16384], P('tensor', 'expert'), may hold values from -0.0625 to 0.0625
- expert_up: bfloat16 [7168, 16384], P('tensor', 'expert'), may hold values from -0.0625 to 0.0625
- expert_down: bfloat16 [16384, 7168], P('expert', 'tensor'), may hold values from -0.1875 to 0.1875
- shared_in: bfloat16 [2, 1024, 7168], P(None, 'expert', 'tensor'), may hold values from -0.0625 to 0.0625
- shared_down: bfloat16 [1024, 7168], P('expert', 'tensor'), may hold values from -0.1875 to 0.1875
Outputs:
- mixed: bfloat16 [8192, 7168], P(('groups', 'expert'), 'tensor'), parts along dimension 0
The draws below stay inside these ranges and needn't reach their ends.
There are 2 independent parts, one for each index of `groups`. The reference program is written for one: setup_inputs(seed, part) draws one part's arguments, and reference() takes and returns one part's arrays. A program takes and returns all parts, laid end to end along the dimension named above; an argument that names none is the same for every part. Nothing has to cross between parts.
Inputs may be any that keep to these rules, and one draw needn't show every extreme that they name: `choices`: within the rows of one index of expert (128 tokens) every expert is named at most 48 times, a bound that some block reaches; a token names 4 different experts.
All inputs are finite; a program needn't handle non-finite values.
Results may differ from the reference program's by a relative error of at most 0.02.
Values may be sent and summed in bfloat16 or wider, within the bound.
No kernel may reach another device: no remote copies, remote signals or barrier semaphores. Data moves between devices by JAX's collectives and lax.ppermute only.
A program may use at most 64 MiB of HBM per device.

```python
import math
import jax
import jax.numpy as jnp
import numpy as np
from jax import lax

D = 7168
FFE = 1024
FS = 1024
EXPERTS = 16
TOP = 4
TOK_DEV = 128
CAP = 48
TOKENS = 4096
PIECE = 512
N_TENSOR = 8


def shard_levels(stream_key, shape, cuts, low, high):
    def one(dim, shards_of):
        draws = jax.random.uniform(jax.random.fold_in(jax.random.fold_in(stream_key, 6), dim), (shards_of,), jnp.float32, low / len(cuts), high / len(cuts))
        return jnp.repeat(jnp.exp(draws), shape[dim] // shards_of).reshape((-1,) + (1,) * (len(shape) - dim - 1))

    factor_of = one(*cuts[0])
    for cut in cuts[1:]:
        factor_of = factor_of * one(*cut)
    return factor_of


def routed_block(own_key, own, number, rows, count, top, limit, skew):
    sequence = jax.random.permutation(own_key, count)
    packed, usual = shares(count, rows * top, limit, skew, True), shares(count, rows * top, limit, skew, False)
    places = jnp.arange(count)

    def named(sizes, rotation):
        used = int((sizes > 0).sum())
        fixed = max(1, used // 4)
        passed = fixed + (places - fixed + rotation * (used - fixed)) % max(1, count - fixed)
        return jnp.zeros((count,), jnp.int32).at[sequence[jnp.where(places < fixed, places, passed)]].set(jnp.asarray(sizes, jnp.int32))

    sizes = jnp.where(number % 4 == 0, named(packed, number // 4), named(usual, number - number // 4 - 1))
    mixed = jax.random.permutation(jax.random.fold_in(own, 3), count)
    donor, taker = mixed[0:count // 2 * 2:2], mixed[1:count // 2 * 2:2]
    margin = jnp.minimum(sizes[donor] - 1, limit - sizes[taker]) // 2
    margin = jnp.where((donor == sequence[0]) | (taker == sequence[0]) | (sizes[taker] == 0), 0, jnp.maximum(margin, 0))
    passed = jax.random.randint(jax.random.fold_in(own, 4), (count // 2,), 0, 1 << 20) % (margin + 1)
    sizes = sizes.at[donor].add(-passed).at[taker].add(passed)
    members = jnp.searchsorted(jnp.cumsum(sizes), jnp.arange(rows * top), side="right").astype(jnp.int32)
    listing = members.reshape(top, rows).T
    listing = listing[jax.random.permutation(jax.random.fold_in(own, 1), rows)]
    rotation = jax.random.randint(jax.random.fold_in(own, 2), (rows, 1), 0, top)
    return jnp.take_along_axis(listing, (jnp.arange(top)[None, :] + rotation) % top, axis=1)


def shares(number_of, total, reach, skew, full):
    loads = [(1 << 20) // math.isqrt(grade ** skew) + 1 for grade in range(1, number_of + 1)]
    largest = reach if full else min(reach, max(-(-total // number_of), total * loads[0] // sum(loads)))
    least = 1 if total - largest >= number_of - 1 else 0
    given, spare = [largest] + [least] * (number_of - 1), total - largest - least * (number_of - 1)
    while spare > 0:
        movable = [i for i in range(1, number_of) if given[i] < largest] or [i for i in range(1, number_of) if given[i] < reach]
        pool, remaining = sum([loads[i] for i in movable]), spare
        for i in movable:
            more = min(reach - given[i], max(1, remaining * loads[i] // pool), spare)
            given[i] = given[i] + more
            spare = spare - more
    return np.array(given)


def noise(own_key, extent, scale, limit, split=(), kind=jnp.bfloat16):
    entries = scale * jax.random.normal(own_key, extent, jnp.float32)
    if split:
        entries = entries * shard_levels(own_key, extent, split, -0.22, 0.18)
    return jnp.clip(entries, -limit, limit).astype(kind)


def setup_inputs(seed: int = 0, part: int = 0) -> dict:
    seeds = jax.random.split(jax.random.key(seed), 9)
    part_keys = jax.random.split(jax.random.fold_in(seeds[8], part), 9)
    tokens = noise(part_keys[0], (TOKENS, D), 1.0, 6.0, ((0, 32), (1, 8)))
    choices_keys = jax.random.split(jax.random.fold_in(part_keys[1], 1), TOKENS // TOK_DEV)
    choices_turns = jax.random.permutation(jax.random.fold_in(part_keys[1], 3), TOKENS // TOK_DEV)
    choices = jax.vmap(lambda own, number: routed_block(jax.random.fold_in(part_keys[1], 2), own, number, TOK_DEV, EXPERTS, TOP, CAP, 2))(choices_keys, choices_turns).reshape((TOKENS, TOP))
    affinity = noise(part_keys[2], (TOKENS, TOP), 1.5, 6.0, ((0, 32),), jnp.float32)
    expert_gate = noise(seeds[3], (D, EXPERTS * FFE), D ** -0.5, 0.0625, ((0, 8), (1, 32)))
    expert_up = noise(seeds[4], (D, EXPERTS * FFE), D ** -0.5, 0.0625, ((0, 8), (1, 32)))
    expert_down = noise(seeds[5], (EXPERTS * FFE, D), FFE ** -0.5, 0.1875, ((0, 32), (1, 8)))
    shared_in = noise(seeds[6], (2, FS, D), D ** -0.5, 0.0625, ((1, 32), (2, 8)))
    shared_down = noise(seeds[7], (FS, D), FS ** -0.5, 0.1875, ((0, 32), (1, 8)))
    return dict(tokens=tokens, choices=choices, affinity=affinity, expert_gate=expert_gate, expert_up=expert_up, expert_down=expert_down, shared_in=shared_in, shared_down=shared_down)


def tensor_partials(feature_slices, weight):
    width = weight.shape[1]
    slices = weight.astype(jnp.float32).reshape(N_TENSOR, D // N_TENSOR, width)
    parts = jnp.einsum("tnd,ndk->ntk", feature_slices, slices, precision=lax.Precision.HIGHEST)
    rounded = lax.optimization_barrier(parts.astype(jnp.bfloat16))
    return jnp.sum(rounded.astype(jnp.float32), axis=0)


def reference(tokens, choices, affinity, expert_gate, expert_up, expert_down, shared_in, shared_down):
    split_count = FFE // PIECE
    feature_slices = tokens.astype(jnp.float32).reshape(TOKENS, N_TENSOR, D // N_TENSOR)
    sigmoids = jax.nn.sigmoid(affinity)
    mix = 2.5 * sigmoids / jnp.sum(sigmoids, axis=1, keepdims=True)
    gate_all = jnp.transpose(expert_gate.reshape(D, EXPERTS, FFE), (1, 0, 2))
    up_all = jnp.transpose(expert_up.reshape(D, EXPERTS, FFE), (1, 0, 2))
    down_all = expert_down.reshape(EXPERTS, split_count, PIECE, D)

    def one_expert(running, inputs):
        gate_cols, up_cols, down_rows, index = inputs
        gate = tensor_partials(feature_slices, gate_cols)
        upper = tensor_partials(feature_slices, up_cols)
        hidden = (jax.nn.silu(gate) * upper).astype(jnp.bfloat16)
        hidden_pieces = hidden.astype(jnp.float32).reshape(TOKENS, split_count, PIECE)
        pieces = jnp.einsum("tsp,spd->tsd", hidden_pieces, down_rows.astype(jnp.float32), precision=lax.Precision.HIGHEST)
        rounded = lax.optimization_barrier(pieces.astype(jnp.bfloat16))
        expert_out = jnp.sum(rounded.astype(jnp.float32), axis=1)
        share = jnp.sum(jnp.where(choices == index, mix, 0.0), axis=1)
        return running + share[:, None] * expert_out, None

    indices = jnp.arange(EXPERTS).astype(jnp.int32)
    start = jnp.zeros((TOKENS, D), jnp.float32)
    routed, unused = lax.scan(one_expert, start, (gate_all, up_all, down_all, indices))
    shared_gate = tensor_partials(feature_slices, jnp.transpose(shared_in[0]))
    shared_up = tensor_partials(feature_slices, jnp.transpose(shared_in[1]))
    shared_hidden = (jax.nn.silu(shared_gate) * shared_up).astype(jnp.bfloat16)
    shared_out = jnp.dot(shared_hidden, shared_down, preferred_element_type=jnp.float32)
    return (routed + shared_out).astype(jnp.bfloat16)
```

```python
import jax
import jax.numpy as jnp
from jax import lax
from jax.sharding import PartitionSpec as P

FFE = 1024
CAP = 48
BF = jnp.bfloat16
F32 = jnp.float32


def dot(spec, a, b):
    return jnp.einsum(spec, a, b, preferred_element_type=F32)


def route(info, columns, top):
    count, _, tok = info.shape
    own = (lax.axis_index("expert") * columns // FFE).astype(F32)
    hit = info[:, :top, :] == own
    named = jnp.any(hit, axis=1)
    weight = jnp.sum(jnp.where(hit, info[:, top:, :], 0.0), axis=1)
    order = jnp.arange(tok)
    before = (order[:, None] < order[None, :]).astype(BF)
    position = dot("ns,st->nt", named.astype(BF), before).astype(jnp.int32)
    slots = jnp.arange(CAP, dtype=jnp.int32)[None, :, None]
    picks = named[:, None, :] & (position[:, None, :] == slots)
    slot_weight = jnp.sum(jnp.where(picks, weight[:, None, :], 0.0), axis=2)
    return picks.astype(BF), slot_weight


def local(tokens, choices, affinity, expert_gate, expert_up, expert_down, shared_in, shared_down):
    tok, width = tokens.shape
    blocks = lax.axis_size("expert")
    parts = lax.axis_size("tensor")
    columns = expert_gate.shape[1]
    units = shared_in.shape[1]
    top = choices.shape[1]
    total = blocks * tok
    sigmoids = jax.nn.sigmoid(affinity)
    mix = 2.5 * sigmoids / jnp.sum(sigmoids, axis=1, keepdims=True)
    info = jnp.concatenate([choices.astype(F32).T, mix.T], axis=0)
    info = lax.all_gather(info, "expert", axis=0)
    picks, slot_weight = route(info, columns, top)
    everyone = lax.all_gather(tokens, "expert", axis=0, tiled=True)
    received = dot("nct,ntd->ncd", picks, everyone.reshape(blocks, tok, width)).astype(BF)
    received = received.reshape(parts, blocks * CAP // parts, width)
    gate = dot("jrd,dp->jrp", received, expert_gate).astype(BF)
    up = dot("jrd,dp->jrp", received, expert_up).astype(BF)
    shared = dot("hd,td->ht", shared_in.reshape(2 * units, width), everyone).astype(BF)
    shared = shared.reshape(2 * units, parts, total // parts).transpose(1, 0, 2)
    slots = blocks * CAP // parts
    sums = lax.psum_scatter(
        jnp.concatenate([gate, up, shared], axis=1), "tensor", scatter_dimension=0, tiled=True
    )[0].astype(F32)
    gates = jnp.concatenate([sums[:slots], sums[2 * slots : 2 * slots + units]], axis=0)
    ups = jnp.concatenate([sums[slots : 2 * slots], sums[2 * slots + units :]], axis=0)
    hidden = (jax.nn.silu(gates) * ups).astype(BF)
    hidden = lax.all_gather(hidden, "tensor", axis=0)
    shared_hidden = hidden[:, slots:].reshape(parts, units, blocks // parts, tok)
    shared_hidden = shared_hidden.transpose(0, 2, 1, 3).reshape(blocks, units, tok)
    produced = dot("rp,pd->rd", hidden[:, :slots].reshape(blocks * CAP, columns), expert_down)
    produced = (produced.reshape(blocks, CAP, width) * slot_weight[:, :, None]).astype(BF)
    values = jnp.concatenate(
        [produced, jnp.broadcast_to(shared_down[None], (blocks, units, width))], axis=1
    )
    share = dot("nkt,nkd->ntd", jnp.concatenate([picks, shared_hidden], axis=1), values)
    return lax.psum_scatter(
        share.astype(BF).reshape(total, width), "expert", scatter_dimension=0, tiled=True
    )


def solution(mesh):
    placed = (
        P(("groups", "expert"), "tensor"),
        P(("groups", "expert"), None),
        P(("groups", "expert"), None),
        P("tensor", "expert"),
        P("tensor", "expert"),
        P("expert", "tensor"),
        P(None, "expert", "tensor"),
        P("expert", "tensor"),
    )
    return jax.shard_map(
        local,
        mesh=mesh,
        in_specs=placed,
        out_specs=P(("groups", "expert"), "tensor"),
        check_vma=False,
    )
```

```python
import jax
import jax.numpy as jnp
from jax import lax
from jax.sharding import PartitionSpec as P

FFE = 1024
CAP = 48
CORES = 2
BF = jnp.bfloat16
F32 = jnp.float32


def dot(spec, a, b):
    return jnp.einsum(spec, a, b, preferred_element_type=F32)


def route(info, columns, top):
    tok = info.shape[2]
    own = (lax.axis_index("expert") * columns // FFE).astype(F32)
    hit = info[:, :top, :] == own
    named = jnp.any(hit, axis=1)
    weight = jnp.sum(jnp.where(hit, info[:, top:, :], 0.0), axis=1)
    order = jnp.arange(tok)
    before = (order[:, None] < order[None, :]).astype(BF)
    position = dot("ns,st->nt", named.astype(BF), before).astype(jnp.int32)
    return jnp.where(named, position, -1), weight


def local(tokens, choices, affinity, expert_gate, expert_up, expert_down, shared_in, shared_down):
    tok, width = tokens.shape
    columns = expert_gate.shape[1]
    units = shared_in.shape[1]
    top = choices.shape[1]
    blocks = lax.axis_size("expert")
    parts = lax.axis_size("tensor")
    pieces = FFE // columns
    near = blocks // pieces
    chips = parts // CORES
    half = CAP // CORES
    core = lax.axis_index("tensor") % CORES
    rings = [[r + pieces * k for k in range(near)] for r in range(pieces)]
    crosses = [[c + CORES * k for k in range(chips)] for c in range(CORES)]
    partner = [(t, t - t % CORES + (t + 1) % CORES) for t in range(parts)]

    def with_mates(array):
        moved = [
            lax.ppermute(
                array, "expert", [(z, z - z % pieces + (z + shift) % pieces) for z in range(blocks)]
            )
            for shift in range(1, pieces)
        ]
        return [array] + moved

    everyone = lax.all_gather(tokens, "expert", axis=0, tiled=True, axis_index_groups=rings)
    gates, ups = with_mates(expert_gate), with_mates(expert_up)
    small = with_mates(jnp.concatenate([shared_in.reshape(2 * units, width), shared_down], axis=0))
    sigmoids = jax.nn.sigmoid(affinity)
    mix = 2.5 * sigmoids / jnp.sum(sigmoids, axis=1, keepdims=True)
    info = jnp.concatenate([choices.astype(F32).T, mix.T], axis=0)
    info = lax.all_gather(info, "expert", axis=0, axis_index_groups=rings)
    slot, weight = route(info, columns, top)
    weights = jnp.concatenate(gates + ups, axis=1)
    shared = jnp.stack([s.reshape(3, units, width) for s in small], axis=1)
    shared = shared.reshape(3, CORES, pieces * units // CORES, width)

    def side(which):
        numbers = which * half + jnp.arange(half, dtype=jnp.int32)
        picks = slot[:, None, :] == numbers[None, :, None]
        slot_weight = jnp.sum(jnp.where(picks, weight[:, None, :], 0.0), axis=2)
        rows = lax.dynamic_index_in_dim(shared, which, axis=1, keepdims=False)
        return picks.astype(BF), slot_weight, rows

    mine, other = side(core), side(1 - core)
    total = near * tok
    rows = near * half // chips
    down, everyone = lax.optimization_barrier((expert_down, everyone))
    downs = jnp.concatenate(with_mates(down), axis=0)

    def sums(picks, shared_rows):
        received = dot("nct,ntd->ncd", picks, everyone.reshape(near, tok, width)).astype(BF)
        routed = dot("jrd,dp->jrp", received.reshape(chips, rows, width), weights).astype(BF)
        wanted = shared_rows[:2].reshape(2, chips, -1, width).transpose(1, 0, 2, 3)
        units_of = dot("hd,td->ht", wanted.reshape(-1, width), everyone).astype(BF)
        units_of = units_of.reshape(chips, -1, total)
        if total != routed.shape[2]:
            units_of = units_of.reshape(chips, -1, routed.shape[2])
        return jnp.concatenate([routed, units_of], axis=1)

    theirs = lax.ppermute(sums(other[0], other[2]), "tensor", partner)
    both = (sums(mine[0], mine[2]).astype(F32) + theirs.astype(F32)).astype(BF)
    crossed = lax.all_to_all(
        both, "tensor", split_axis=0, concat_axis=0, tiled=True, axis_index_groups=crosses
    )
    summed = jnp.sum(crossed.astype(F32), axis=0)
    routed = summed[:rows]
    pair = summed[rows:].reshape(2, -1, total)
    routed = (jax.nn.silu(routed[:, :FFE]) * routed[:, FFE:]).astype(BF)
    shared_hidden = (jax.nn.silu(pair[0]) * pair[1]).astype(BF).reshape(-1, FFE)
    hidden = jnp.concatenate([routed, shared_hidden], axis=0)
    hidden = lax.all_gather(hidden, "tensor", axis=0, axis_index_groups=crosses)
    their_hidden = lax.ppermute(hidden, "tensor", partner)

    def outs(hidden, slot_weight):
        out = dot("rp,pd->rd", hidden[:, :rows].reshape(near * half, FFE), downs)
        out = (out.reshape(near, half, width) * slot_weight[:, :, None]).astype(BF)
        units_of = hidden[:, rows:].reshape(-1, near, tok).transpose(1, 0, 2)
        return out, units_of

    (out_a, units_a), (out_b, units_b) = outs(hidden, mine[1]), outs(their_hidden, other[1])
    spread = [
        jnp.broadcast_to(s[2][2], (near, *s[2].shape[1:])) for s in (mine, other)
    ]
    share = dot(
        "nkt,nkd->ntd",
        jnp.concatenate([mine[0], other[0], units_a, units_b], axis=1),
        jnp.concatenate([out_a, out_b, *spread], axis=1),
    )
    return lax.psum_scatter(
        share.astype(BF).reshape(total, width),
        "expert",
        scatter_dimension=0,
        tiled=True,
        axis_index_groups=rings,
    )


def solution(mesh):
    placed = (
        P(("groups", "expert"), "tensor"),
        P(("groups", "expert"), None),
        P(("groups", "expert"), None),
        P("tensor", "expert"),
        P("tensor", "expert"),
        P("expert", "tensor"),
        P(None, "expert", "tensor"),
        P("expert", "tensor"),
    )
    return jax.shard_map(
        local,
        mesh=mesh,
        in_specs=placed,
        out_specs=P(("groups", "expert"), "tensor"),
        check_vma=False,
    )
```

```python
import jax
import jax.numpy as jnp
from jax import lax
from jax.sharding import PartitionSpec as P

FFE = 1024
CAP = 48
CORES = 2
OFFLOADED = 4
BF = jnp.bfloat16
F32 = jnp.float32


def dot(spec, a, b):
    return jnp.einsum(spec, a, b, preferred_element_type=F32)


def route(info, columns, top):
    tok = info.shape[2]
    own = (lax.axis_index("expert") * columns // FFE).astype(F32)
    hit = info[:, :top, :] == own
    named = jnp.any(hit, axis=1)
    weight = jnp.sum(jnp.where(hit, info[:, top:, :], 0.0), axis=1)
    order = jnp.arange(tok)
    before = (order[:, None] < order[None, :]).astype(BF)
    position = dot("ns,st->nt", named.astype(BF), before).astype(jnp.int32)
    return jnp.where(named, position, -1), weight


def local(tokens, choices, affinity, expert_gate, expert_up, expert_down, shared_in, shared_down):
    tok, width = tokens.shape
    columns = expert_gate.shape[1]
    units = shared_in.shape[1]
    top = choices.shape[1]
    blocks = lax.axis_size("expert")
    parts = lax.axis_size("tensor")
    pieces = FFE // columns
    near = blocks // pieces
    chips = parts // CORES
    half = CAP // CORES
    core = lax.axis_index("tensor") % CORES
    rings = [[r + pieces * k for k in range(near)] for r in range(pieces)]
    crosses = [[c + CORES * k for k in range(chips)] for c in range(CORES)]
    partner = [(t, t - t % CORES + (t + 1) % CORES) for t in range(parts)]

    def with_mates(array):
        moved = [
            lax.ppermute(
                array, "expert", [(z, z - z % pieces + (z + shift) % pieces) for z in range(blocks)]
            )
            for shift in range(1, pieces)
        ]
        return [array] + moved

    def scatter_ring(share):
        place = lax.axis_index("expert") // pieces
        far = near // 2
        onward = [(z, (z + pieces) % blocks) for z in range(blocks)]
        backward = [(z, (z - pieces) % blocks) for z in range(blocks)]

        def own(offset):
            return lax.dynamic_index_in_dim(share, (place + offset) % near, 0, False).astype(F32)

        ahead, back = own(far).astype(BF), own(1 - far).astype(BF)
        for step in range(far):
            ahead = lax.ppermute(ahead, "expert", onward)
            if step < far - 1:
                back = lax.ppermute(back, "expert", backward)
                ahead = (ahead.astype(F32) + own(far - 1 - step)).astype(BF)
            if step < far - 2:
                back = (back.astype(F32) + own(step + 2 - far)).astype(BF)
        return (own(0) + ahead.astype(F32) + back.astype(F32)).astype(BF)

    everyone = lax.all_gather(tokens, "expert", axis=0, tiled=True, axis_index_groups=rings)
    sigmoids = jax.nn.sigmoid(affinity)
    mix = 2.5 * sigmoids / jnp.sum(sigmoids, axis=1, keepdims=True)
    info = jnp.concatenate([choices.astype(F32).T, mix.T], axis=0)
    info = lax.all_to_all(
        jnp.broadcast_to(info[None], (near, *info.shape)),
        "expert",
        split_axis=0,
        concat_axis=0,
        tiled=True,
        axis_index_groups=rings,
    )
    gate_up = jnp.concatenate([shared_in.reshape(2 * units, width), shared_down], axis=0)
    info, gate, up, small = lax.optimization_barrier((info, expert_gate, expert_up, gate_up))
    small, gates, ups = with_mates(small), with_mates(gate), with_mates(up)
    slot, weight = route(info, columns, top)
    weights = jnp.concatenate(gates + ups, axis=1)
    shared = jnp.stack([s.reshape(3, units, width) for s in small], axis=1)
    shared = shared.reshape(3, CORES, pieces * units // CORES, width)

    def side(which):
        numbers = which * half + jnp.arange(half, dtype=jnp.int32)
        picks = slot[:, None, :] == numbers[None, :, None]
        slot_weight = jnp.sum(jnp.where(picks, weight[:, None, :], 0.0), axis=2)
        rows = lax.dynamic_index_in_dim(shared, which, axis=1, keepdims=False)
        return picks.astype(BF), slot_weight, rows

    mine, other = side(core), side(1 - core)
    total = near * tok
    rows = near * half // chips
    down, everyone = lax.optimization_barrier((expert_down, everyone))
    downs = jnp.concatenate(with_mates(down), axis=0)

    def sums(picks, shared_rows):
        received = dot("nct,ntd->ncd", picks, everyone.reshape(near, tok, width)).astype(BF)
        routed = dot("jrd,dp->jrp", received.reshape(chips, rows, width), weights).astype(BF)
        wanted = shared_rows[:2].reshape(2, chips, -1, width).transpose(1, 0, 2, 3)
        units_of = dot("hd,td->ht", wanted.reshape(-1, width), everyone).astype(BF)
        units_of = units_of.reshape(chips, -1, total)
        if total != routed.shape[2]:
            units_of = units_of.reshape(chips, -1, routed.shape[2])
        return jnp.concatenate([routed, units_of], axis=1)

    theirs = lax.ppermute(sums(other[0], other[2]), "tensor", partner)
    both = (sums(mine[0], mine[2]).astype(F32) + theirs.astype(F32)).astype(BF)
    crossed = lax.all_to_all(
        both, "tensor", split_axis=0, concat_axis=0, tiled=True, axis_index_groups=crosses
    )
    summed = jnp.sum(crossed.astype(F32), axis=0)
    routed = summed[:rows]
    pair = summed[rows:].reshape(2, -1, total)
    routed = (jax.nn.silu(routed[:, :FFE]) * routed[:, FFE:]).astype(BF)
    shared_hidden = (jax.nn.silu(pair[0]) * pair[1]).astype(BF).reshape(-1, FFE)
    hidden = jnp.concatenate([routed, shared_hidden], axis=0)
    hidden = lax.all_gather(hidden, "tensor", axis=0, axis_index_groups=crosses)
    their_hidden = lax.ppermute(hidden, "tensor", partner)

    def outs(hidden, slot_weight):
        out = dot("rp,pd->rd", hidden[:, :rows].reshape(near * half, FFE), downs)
        out = (out.reshape(near, half, width) * slot_weight[:, :, None]).astype(BF)
        units_of = hidden[:, rows:].reshape(-1, near, tok).transpose(1, 0, 2)
        return out, units_of

    (out_a, units_a), (out_b, units_b) = outs(hidden, mine[1]), outs(their_hidden, other[1])
    spread = [
        jnp.broadcast_to(s[2][2], (near, *s[2].shape[1:])) for s in (mine, other)
    ]
    takers = jnp.concatenate([mine[0], other[0], units_a, units_b], axis=1)

    def share(low, high):
        values = jnp.concatenate([v[:, :, low:high] for v in (out_a, out_b, *spread)], axis=1)
        return dot("nkt,nkd->ntd", takers, values).astype(BF)

    cut = OFFLOADED * width // 7
    first = lax.psum_scatter(
        share(0, cut).reshape(total, cut),
        "expert",
        scatter_dimension=0,
        tiled=True,
        axis_index_groups=rings,
    )
    return jnp.concatenate([first, scatter_ring(share(cut, width))], axis=1)


def solution(mesh):
    placed = (
        P(("groups", "expert"), "tensor"),
        P(("groups", "expert"), None),
        P(("groups", "expert"), None),
        P("tensor", "expert"),
        P("tensor", "expert"),
        P("expert", "tensor"),
        P(None, "expert", "tensor"),
        P("expert", "tensor"),
    )
    return jax.shard_map(
        local,
        mesh=mesh,
        in_specs=placed,
        out_specs=P(("groups", "expert"), "tensor"),
        check_vma=False,
    )
```

```python
import jax
import jax.numpy as jnp
from jax import lax
from jax.sharding import PartitionSpec as P


FFE = 1024
CAP = 48
CORES = 2
BF = jnp.bfloat16
F32 = jnp.float32


def dot(spec, a, b):
    return jnp.einsum(spec, a, b, preferred_element_type=F32)


def route(info, columns, top):
    tok = info.shape[2]
    own = (lax.axis_index("expert") * columns // FFE).astype(F32)
    hit = info[:, :top, :] == own
    named = jnp.any(hit, axis=1)
    weight = jnp.sum(jnp.where(hit, info[:, top:, :], 0.0), axis=1)
    order = jnp.arange(tok)
    before = (order[:, None] < order[None, :]).astype(BF)
    position = dot("ns,st->nt", named.astype(BF), before).astype(jnp.int32)
    return jnp.where(named, position, -1), weight


def local(tokens, choices, affinity, expert_gate, expert_up, expert_down, shared_in, shared_down):
    tok, width = tokens.shape
    columns = expert_gate.shape[1]
    units = shared_in.shape[1]
    top = choices.shape[1]
    blocks = lax.axis_size("expert")
    parts = lax.axis_size("tensor")
    pieces = FFE // columns
    near = blocks // pieces
    chips = parts // CORES
    half = CAP // CORES
    core = lax.axis_index("tensor") % CORES
    rings = [[r + pieces * k for k in range(near)] for r in range(pieces)]
    crosses = [[c + CORES * k for k in range(chips)] for c in range(CORES)]
    partner = [(t, t - t % CORES + (t + 1) % CORES) for t in range(parts)]

    def with_mates(array):
        moved = [
            lax.ppermute(
                array, "expert", [(z, z - z % pieces + (z + shift) % pieces) for z in range(blocks)]
            )
            for shift in range(1, pieces)
        ]
        return [array] + moved

    everyone = lax.all_gather(tokens, "expert", axis=0, tiled=True, axis_index_groups=rings)
    sigmoids = jax.nn.sigmoid(affinity)
    mix = 2.5 * sigmoids / jnp.sum(sigmoids, axis=1, keepdims=True)
    info = jnp.concatenate([choices.astype(F32).T, mix.T], axis=0)
    info = lax.all_to_all(
        jnp.broadcast_to(info[None], (near, *info.shape)),
        "expert",
        split_axis=0,
        concat_axis=0,
        tiled=True,
        axis_index_groups=rings,
    )
    small = jnp.concatenate([shared_in.reshape(2 * units, width), shared_down], axis=0)
    smalls = with_mates(small)
    gates = with_mates(expert_gate)
    ups = with_mates(expert_up)
    slot, weight = route(info, columns, top)
    shared = jnp.stack([s.reshape(3, units, width) for s in smalls], axis=1)
    shared = shared.reshape(3, CORES, pieces * units // CORES, width)

    def side(which):
        numbers = which * half + jnp.arange(half, dtype=jnp.int32)
        picks = slot[:, None, :] == numbers[None, :, None]
        slot_weight = jnp.sum(jnp.where(picks, weight[:, None, :], 0.0), axis=2)
        rows = lax.dynamic_index_in_dim(shared, which, axis=1, keepdims=False)
        return picks.astype(BF), slot_weight, rows

    sides = side(core), side(1 - core)
    total = near * tok
    rows = near * half // chips
    down, everyone = lax.optimization_barrier((expert_down, everyone))
    downs = with_mates(down)

    def partials(which, piece, everyone):
        picks, _, shared_rows = sides[which]
        received = dot("nct,ntd->ncd", picks, everyone.reshape(near, tok, width)).astype(BF)
        weights = jnp.concatenate([gates[piece], ups[piece]], axis=1)
        routed = dot("jrd,dp->jrp", received.reshape(chips, rows, width), weights).astype(BF)
        if piece:
            return routed
        wanted = shared_rows[:2].reshape(2, chips, -1, width).transpose(1, 0, 2, 3)
        units_of = dot("hd,td->ht", wanted.reshape(-1, width), everyone).astype(BF)
        return jnp.concatenate([routed, units_of.reshape(chips, -1, 2 * columns)], axis=1)

    crossed, hiddens = [], []
    for piece in range(pieces):
        if piece:
            _, everyone = lax.optimization_barrier((sent, everyone))
        theirs = lax.ppermute(partials(1, piece, everyone), "tensor", partner)
        sent = (partials(0, piece, everyone).astype(F32) + theirs.astype(F32)).astype(BF)
        taken = lax.all_to_all(
            sent, "tensor", split_axis=0, concat_axis=0, tiled=True, axis_index_groups=crosses
        )
        crossed.append(taken)
    for piece in range(pieces):
        summed = jnp.sum(crossed[piece].astype(F32), axis=0)
        routed = summed[:rows]
        hidden = (jax.nn.silu(routed[:, :columns]) * routed[:, columns:]).astype(BF)
        if not piece:
            pair = summed[rows:].reshape(2, -1, total)
            shared_hidden = (jax.nn.silu(pair[0]) * pair[1]).astype(BF).reshape(-1, columns)
            hidden = jnp.concatenate([hidden, shared_hidden], axis=0)
        hidden = lax.all_to_all(
            jnp.broadcast_to(hidden[None], (chips, *hidden.shape)),
            "tensor",
            split_axis=0,
            concat_axis=0,
            tiled=True,
            axis_index_groups=crosses,
        )
        hiddens.append((hidden, lax.ppermute(hidden, "tensor", partner)))
    takers, values = [], []
    for which, (picks, slot_weight, _) in enumerate(sides):
        out = sum(
            dot("rp,pd->rd", h[which][:, :rows].reshape(near * half, columns), d)
            for h, d in zip(hiddens, downs)
        )
        takers.append(picks)
        values.append((out.reshape(near, half, width) * slot_weight[:, :, None]).astype(BF))
    for h, (_, _, shared_rows) in zip(hiddens[0], sides):
        takers.append(h[:, rows:].reshape(-1, near, tok).transpose(1, 0, 2))
        values.append(jnp.broadcast_to(shared_rows[2][None], (near, *shared_rows.shape[1:])))
    share = dot(
        "nkt,nkd->ntd", jnp.concatenate(takers, axis=1), jnp.concatenate(values, axis=1)
    )
    return lax.psum_scatter(
        share.astype(BF).reshape(total, width),
        "expert",
        scatter_dimension=0,
        tiled=True,
        axis_index_groups=rings,
    )


def solution(mesh):
    placed = (
        P(("groups", "expert"), "tensor"),
        P(("groups", "expert"), None),
        P(("groups", "expert"), None),
        P("tensor", "expert"),
        P("tensor", "expert"),
        P("expert", "tensor"),
        P(None, "expert", "tensor"),
        P("expert", "tensor"),
    )

    return jax.shard_map(
        local,
        mesh=mesh,
        in_specs=placed,
        out_specs=P(("groups", "expert"), "tensor"),
        check_vma=False,
    )
```

```python
import jax
import jax.numpy as jnp
from jax import lax
from jax.sharding import PartitionSpec as P


FFE = 1024
CAP = 48
CORES = 2
BF = jnp.bfloat16
F32 = jnp.float32


def dot(spec, a, b):
    return jnp.einsum(spec, a, b, preferred_element_type=F32)


def route(info, columns, top):
    tok = info.shape[2]
    own = (lax.axis_index("expert") * columns // FFE).astype(F32)
    hit = info[:, :top, :] == own
    named = jnp.any(hit, axis=1)
    weight = jnp.sum(jnp.where(hit, info[:, top:, :], 0.0), axis=1)
    order = jnp.arange(tok)
    before = (order[:, None] < order[None, :]).astype(BF)
    position = dot("ns,st->nt", named.astype(BF), before).astype(jnp.int32)
    return jnp.where(named, position, -1), weight


def local(tokens, choices, affinity, expert_gate, expert_up, expert_down, shared_in, shared_down):
    tok, width = tokens.shape
    columns = expert_gate.shape[1]
    units = shared_in.shape[1]
    top = choices.shape[1]
    blocks = lax.axis_size("expert")
    parts = lax.axis_size("tensor")
    pieces = FFE // columns
    near = blocks // pieces
    chips = parts // CORES
    half = CAP // CORES
    core = lax.axis_index("tensor") % CORES
    rings = [[r + pieces * k for k in range(near)] for r in range(pieces)]
    crosses = [[c + CORES * k for k in range(chips)] for c in range(CORES)]
    partner = [(t, t - t % CORES + (t + 1) % CORES) for t in range(parts)]

    def with_mates(array):
        moved = [
            lax.ppermute(
                array, "expert", [(z, z - z % pieces + (z + shift) % pieces) for z in range(blocks)]
            )
            for shift in range(1, pieces)
        ]
        return [array] + moved

    everyone = lax.all_gather(tokens, "expert", axis=0, tiled=True, axis_index_groups=rings)
    gates = with_mates(expert_gate)
    ups = with_mates(expert_up)
    small = with_mates(jnp.concatenate([shared_in.reshape(2 * units, width), shared_down], axis=0))
    sigmoids = jax.nn.sigmoid(affinity)
    mix = 2.5 * sigmoids / jnp.sum(sigmoids, axis=1, keepdims=True)
    info = jnp.concatenate([choices.astype(F32).T, mix.T], axis=0)
    info = lax.all_to_all(
        jnp.broadcast_to(info[None], (near, *info.shape)),
        "expert",
        split_axis=0,
        concat_axis=0,
        tiled=True,
        axis_index_groups=rings,
    )
    slot, weight = route(info, columns, top)
    weights = jnp.concatenate(gates + ups, axis=1)
    shared = jnp.stack([s.reshape(3, units, width) for s in small], axis=1)
    shared = shared.reshape(3, CORES, pieces * units // CORES, width)

    def side(which):
        numbers = which * half + jnp.arange(half, dtype=jnp.int32)
        picks = slot[:, None, :] == numbers[None, :, None]
        slot_weight = jnp.sum(jnp.where(picks, weight[:, None, :], 0.0), axis=2)
        rows = lax.dynamic_index_in_dim(shared, which, axis=1, keepdims=False)
        return picks.astype(BF), slot_weight, rows

    mine, other = side(core), side(1 - core)
    total = near * tok
    rows = near * half // chips
    down, everyone = lax.optimization_barrier((expert_down, everyone))
    downs = jnp.concatenate(with_mates(down), axis=0)

    def sums(picks, shared_rows):
        received = dot("nct,ntd->ncd", picks, everyone.reshape(near, tok, width)).astype(BF)
        routed = dot("jrd,dp->jrp", received.reshape(chips, rows, width), weights).astype(BF)
        wanted = shared_rows[:2].reshape(2, chips, -1, width).transpose(1, 0, 2, 3)
        units_of = dot("hd,td->ht", wanted.reshape(-1, width), everyone).astype(BF)
        units_of = units_of.reshape(chips, -1, total)
        if total != routed.shape[2]:
            units_of = units_of.reshape(chips, -1, routed.shape[2])
        return jnp.concatenate([routed, units_of], axis=1)

    theirs = lax.ppermute(sums(other[0], other[2]), "tensor", partner)
    both = (sums(mine[0], mine[2]).astype(F32) + theirs.astype(F32)).astype(BF)
    chip = lax.axis_index("tensor") // CORES
    summed = 0.0
    for shift in (*range(1, chips), 0):
        term = lax.dynamic_index_in_dim(both, (chip + shift) % chips, keepdims=False)
        if shift:
            hop = [(t, (t + CORES * shift) % parts) for t in range(parts)]
            term = lax.ppermute(term, "tensor", hop)
        summed = summed + term.astype(F32)
    routed = summed[:rows]
    pair = summed[rows:].reshape(2, -1, total)
    routed = (jax.nn.silu(routed[:, :FFE]) * routed[:, FFE:]).astype(BF)
    shared_hidden = (jax.nn.silu(pair[0]) * pair[1]).astype(BF).reshape(-1, FFE)
    hidden = jnp.concatenate([routed, shared_hidden], axis=0)
    hidden = lax.all_gather(hidden, "tensor", axis=0, axis_index_groups=crosses)
    their_hidden = lax.ppermute(hidden, "tensor", partner)

    def outs(hidden, slot_weight):
        out = dot("rp,pd->rd", hidden[:, :rows].reshape(near * half, FFE), downs)
        out = (out.reshape(near, half, width) * slot_weight[:, :, None]).astype(BF)
        units_of = hidden[:, rows:].reshape(-1, near, tok).transpose(1, 0, 2)
        return out, units_of

    (out_a, units_a), (out_b, units_b) = outs(hidden, mine[1]), outs(their_hidden, other[1])
    spread = [
        jnp.broadcast_to(s[2][2], (near, *s[2].shape[1:])) for s in (mine, other)
    ]
    share = dot(
        "nkt,nkd->ntd",
        jnp.concatenate([mine[0], other[0], units_a, units_b], axis=1),
        jnp.concatenate([out_a, out_b, *spread], axis=1),
    )
    return lax.psum_scatter(
        share.astype(BF).reshape(total, width),
        "expert",
        scatter_dimension=0,
        tiled=True,
        axis_index_groups=rings,
    )


def solution(mesh):
    placed = (
        P(("groups", "expert"), "tensor"),
        P(("groups", "expert"), None),
        P(("groups", "expert"), None),
        P("tensor", "expert"),
        P("tensor", "expert"),
        P("expert", "tensor"),
        P(None, "expert", "tensor"),
        P("expert", "tensor"),
    )

    return jax.shard_map(
        local,
        mesh=mesh,
        in_specs=placed,
        out_specs=P(("groups", "expert"), "tensor"),
        check_vma=False,
    )
```

```python
import jax
import jax.numpy as jnp
from jax import lax
from jax.sharding import PartitionSpec as P


FFE = 1024
CAP = 48
CORES = 2
BF = jnp.bfloat16
F32 = jnp.float32


def dot(spec, a, b):
    return jnp.einsum(spec, a, b, preferred_element_type=F32)


def route(info, columns, top):
    tok = info.shape[2]
    own = (lax.axis_index("expert") * columns // FFE).astype(F32)
    hit = info[:, :top, :] == own
    named = jnp.any(hit, axis=1)
    weight = jnp.sum(jnp.where(hit, info[:, top:, :], 0.0), axis=1)
    order = jnp.arange(tok)
    before = (order[:, None] < order[None, :]).astype(BF)
    position = dot("ns,st->nt", named.astype(BF), before).astype(jnp.int32)
    return jnp.where(named, position, -1), weight


def local(tokens, choices, affinity, expert_gate, expert_up, expert_down, shared_in, shared_down):
    tok, width = tokens.shape
    columns = expert_gate.shape[1]
    units = shared_in.shape[1]
    top = choices.shape[1]
    blocks = lax.axis_size("expert")
    parts = lax.axis_size("tensor")
    pieces = FFE // columns
    near = blocks // pieces
    chips = parts // CORES
    half = CAP // CORES
    core = lax.axis_index("tensor") % CORES
    rings = [[r + pieces * k for k in range(near)] for r in range(pieces)]
    crosses = [[c + CORES * k for k in range(chips)] for c in range(CORES)]
    partner = [(t, t - t % CORES + (t + 1) % CORES) for t in range(parts)]

    def with_mates(array):
        moved = [
            lax.ppermute(
                array, "expert", [(z, z - z % pieces + (z + shift) % pieces) for z in range(blocks)]
            )
            for shift in range(1, pieces)
        ]
        return [array] + moved

    everyone = lax.all_gather(tokens, "expert", axis=0, tiled=True, axis_index_groups=rings)
    gates = with_mates(expert_gate)
    small = jnp.concatenate([shared_in.reshape(2 * units, width), shared_down], axis=0)
    small = with_mates(small)
    sigmoids = jax.nn.sigmoid(affinity)
    mix = 2.5 * sigmoids / jnp.sum(sigmoids, axis=1, keepdims=True)
    info = jnp.concatenate([choices.astype(F32).T, mix.T], axis=0)
    info = lax.all_to_all(
        jnp.broadcast_to(info[None], (near, *info.shape)),
        "expert",
        split_axis=0,
        concat_axis=0,
        tiled=True,
        axis_index_groups=rings,
    )
    slot, weight = route(info, columns, top)
    shared = jnp.stack([s.reshape(3, units, width) for s in small], axis=1)
    shared = shared.reshape(3, CORES, pieces * units // CORES, width)

    def side(which):
        numbers = which * half + jnp.arange(half, dtype=jnp.int32)
        picks = slot[:, None, :] == numbers[None, :, None]
        slot_weight = jnp.sum(jnp.where(picks, weight[:, None, :], 0.0), axis=2)
        rows = lax.dynamic_index_in_dim(shared, which, axis=1, keepdims=False)
        return picks.astype(BF), slot_weight, rows

    mine, other = side(core), side(1 - core)
    total = near * tok
    rows = near * half // chips
    late_up, down, everyone = lax.optimization_barrier((expert_up, expert_down, everyone))
    ups = with_mates(late_up)
    downs = jnp.concatenate(with_mates(down), axis=0)
    received = [
        dot("nct,ntd->ncd", picks, everyone.reshape(near, tok, width))
        .astype(BF)
        .reshape(chips, rows, width)
        for picks, _, _ in (mine, other)
    ]
    chip = lax.axis_index("tensor") // CORES

    def first(which):
        weights = jnp.concatenate([*gates, expert_up], axis=1)
        return dot("jrd,dp->jrp", received[which], weights).astype(BF)

    def second(which):
        late = [dot("jrd,dp->jrp", received[which], up).astype(BF) for up in ups[1:]]
        shared_rows = (mine, other)[which][2]
        wanted = shared_rows[:2].reshape(2, chips, -1, width).transpose(1, 0, 2, 3)
        units_of = dot("hd,td->ht", wanted.reshape(-1, width), everyone).astype(BF)
        return jnp.concatenate([*late, units_of.reshape(chips, -1, columns)], axis=1)

    def summed(partials):
        theirs = lax.ppermute(partials(1), "tensor", partner)
        both = (partials(0).astype(F32) + theirs.astype(F32)).astype(BF)
        total_of = lax.dynamic_index_in_dim(both, chip, keepdims=False).astype(F32)
        for shift in range(1, chips):
            term = lax.dynamic_index_in_dim(both, (chip + shift) % chips, keepdims=False)
            hop = [(t, (t + CORES * shift) % parts) for t in range(parts)]
            term = lax.ppermute(term, "tensor", hop)
            total_of = total_of + term.astype(F32)
        return total_of

    early, late = summed(first), summed(second)
    gate_of, up_of = early[:, :FFE], [early[:, FFE:]]
    up_of += [late[rows * p : rows * (p + 1)] for p in range(pieces - 1)]
    pair = late[rows * (pieces - 1) :].reshape(2, -1, total)
    routed = [
        (jax.nn.silu(gate_of[:, columns * p : columns * (p + 1)]) * up_of[p]).astype(BF)
        for p in range(pieces)
    ]
    routed = jnp.concatenate(routed, axis=1)
    shared_hidden = (jax.nn.silu(pair[0]) * pair[1]).astype(BF).reshape(-1, FFE)
    hidden = jnp.concatenate([routed, shared_hidden], axis=0)
    hidden = lax.all_gather(hidden, "tensor", axis=0, axis_index_groups=crosses)
    their_hidden = lax.ppermute(hidden, "tensor", partner)

    def outs(hidden, slot_weight):
        out = dot("rp,pd->rd", hidden[:, :rows].reshape(near * half, FFE), downs)
        out = (out.reshape(near, half, width) * slot_weight[:, :, None]).astype(BF)
        units_of = hidden[:, rows:].reshape(-1, near, tok).transpose(1, 0, 2)
        return out, units_of

    (out_a, units_a), (out_b, units_b) = outs(hidden, mine[1]), outs(their_hidden, other[1])
    spread = [
        jnp.broadcast_to(s[2][2], (near, *s[2].shape[1:])) for s in (mine, other)
    ]
    share = dot(
        "nkt,nkd->ntd",
        jnp.concatenate([mine[0], other[0], units_a, units_b], axis=1),
        jnp.concatenate([out_a, out_b, *spread], axis=1),
    )
    return lax.psum_scatter(
        share.astype(BF).reshape(total, width),
        "expert",
        scatter_dimension=0,
        tiled=True,
        axis_index_groups=rings,
    )


def solution(mesh):
    placed = (
        P(("groups", "expert"), "tensor"),
        P(("groups", "expert"), None),
        P(("groups", "expert"), None),
        P("tensor", "expert"),
        P("tensor", "expert"),
        P("expert", "tensor"),
        P(None, "expert", "tensor"),
        P("expert", "tensor"),
    )

    return jax.shard_map(
        local,
        mesh=mesh,
        in_specs=placed,
        out_specs=P(("groups", "expert"), "tensor"),
        check_vma=False,
    )
```

```python
import jax
import jax.numpy as jnp
from jax import lax
from jax.sharding import PartitionSpec as P


FFE = 1024
CAP = 48
CORES = 2
BF = jnp.bfloat16
F32 = jnp.float32


def dot(spec, a, b):
    return jnp.einsum(spec, a, b, preferred_element_type=F32)


def route(info, columns, top):
    tok = info.shape[2]
    own = (lax.axis_index("expert") * columns // FFE).astype(F32)
    hit = info[:, :top, :] == own
    named = jnp.any(hit, axis=1)
    weight = jnp.sum(jnp.where(hit, info[:, top:, :], 0.0), axis=1)
    order = jnp.arange(tok)
    before = (order[:, None] < order[None, :]).astype(BF)
    position = dot("ns,st->nt", named.astype(BF), before).astype(jnp.int32)
    return jnp.where(named, position, -1), weight


def local(tokens, choices, affinity, expert_gate, expert_up, expert_down, shared_in, shared_down):
    tok, width = tokens.shape
    columns = expert_gate.shape[1]
    units = shared_in.shape[1]
    top = choices.shape[1]
    blocks = lax.axis_size("expert")
    parts = lax.axis_size("tensor")
    pieces = FFE // columns
    near = blocks // pieces
    chips = parts // CORES
    half = CAP // CORES
    core = lax.axis_index("tensor") % CORES
    rings = [[r + pieces * k for k in range(near)] for r in range(pieces)]
    crosses = [[c + CORES * k for k in range(chips)] for c in range(CORES)]
    partner = [(t, t - t % CORES + (t + 1) % CORES) for t in range(parts)]

    def with_mates(array):
        moved = [
            lax.ppermute(
                array, "expert", [(z, z - z % pieces + (z + shift) % pieces) for z in range(blocks)]
            )
            for shift in range(1, pieces)
        ]
        return [array] + moved

    everyone = lax.all_gather(tokens, "expert", axis=0, tiled=True, axis_index_groups=rings)
    gates = with_mates(expert_gate)
    small = jnp.concatenate([shared_in.reshape(2 * units, width), shared_down], axis=0)
    small = with_mates(small)
    sigmoids = jax.nn.sigmoid(affinity)
    mix = 2.5 * sigmoids / jnp.sum(sigmoids, axis=1, keepdims=True)
    info = jnp.concatenate([choices.astype(F32).T, mix.T], axis=0)
    info = lax.all_to_all(
        jnp.broadcast_to(info[None], (near, *info.shape)),
        "expert",
        split_axis=0,
        concat_axis=0,
        tiled=True,
        axis_index_groups=rings,
    )
    slot, weight = route(info, columns, top)
    shared = jnp.stack([s.reshape(3, units, width) for s in small], axis=1)
    shared = shared.reshape(3, CORES, pieces * units // CORES, width)

    def side(which):
        numbers = which * half + jnp.arange(half, dtype=jnp.int32)
        picks = slot[:, None, :] == numbers[None, :, None]
        slot_weight = jnp.sum(jnp.where(picks, weight[:, None, :], 0.0), axis=2)
        rows = lax.dynamic_index_in_dim(shared, which, axis=1, keepdims=False)
        return picks.astype(BF), slot_weight, rows

    mine, other = side(core), side(1 - core)
    total = near * tok
    rows = near * half // chips
    late_up, down, everyone = lax.optimization_barrier((expert_up, expert_down, everyone))
    ups = with_mates(late_up)
    downs = jnp.concatenate(with_mates(down), axis=0)
    received = [
        dot("nct,ntd->ncd", picks, everyone.reshape(near, tok, width))
        .astype(BF)
        .reshape(chips, rows, width)
        for picks, _, _ in (mine, other)
    ]
    wanted = jnp.stack([side_of[2][:2] for side_of in (mine, other)])
    wanted = wanted.reshape(CORES, 2, chips, -1, width).transpose(0, 2, 1, 3, 4)
    shared_sums = dot("hd,td->ht", wanted.reshape(-1, width), everyone).astype(BF)
    shared_sums = shared_sums.reshape(CORES, chips, -1, columns)

    def first(which):
        weights = jnp.concatenate([*gates, expert_up], axis=1)
        return dot("jrd,dp->jrp", received[which], weights).astype(BF)

    def second(which):
        late = [dot("jrd,dp->jrp", received[which], up).astype(BF) for up in ups[1:]]
        return jnp.concatenate([*late, shared_sums[which]], axis=1)

    def summed(partials):
        theirs = lax.ppermute(partials(1), "tensor", partner)
        both = (partials(0).astype(F32) + theirs.astype(F32)).astype(BF)
        crossed = lax.all_to_all(
            both, "tensor", split_axis=0, concat_axis=0, tiled=True, axis_index_groups=crosses
        )
        return jnp.sum(crossed.astype(F32), axis=0)

    early, late = summed(first), summed(second)
    gate_of, up_of = early[:, :FFE], [early[:, FFE:]]
    up_of += [late[rows * p : rows * (p + 1)] for p in range(pieces - 1)]
    pair = late[rows * (pieces - 1) :].reshape(2, -1, total)
    routed = [
        (jax.nn.silu(gate_of[:, columns * p : columns * (p + 1)]) * up_of[p]).astype(BF)
        for p in range(pieces)
    ]
    routed = jnp.concatenate(routed, axis=1)
    shared_hidden = (jax.nn.silu(pair[0]) * pair[1]).astype(BF).reshape(-1, FFE)
    hidden = jnp.concatenate([routed, shared_hidden], axis=0)
    hidden = lax.all_gather(hidden, "tensor", axis=0, axis_index_groups=crosses)
    their_hidden = lax.ppermute(hidden, "tensor", partner)

    def outs(hidden, slot_weight):
        out = dot("rp,pd->rd", hidden[:, :rows].reshape(near * half, FFE), downs)
        out = (out.reshape(near, half, width) * slot_weight[:, :, None]).astype(BF)
        units_of = hidden[:, rows:].reshape(-1, near, tok).transpose(1, 0, 2)
        return out, units_of

    (out_a, units_a), (out_b, units_b) = outs(hidden, mine[1]), outs(their_hidden, other[1])
    spread = [
        jnp.broadcast_to(s[2][2], (near, *s[2].shape[1:])) for s in (mine, other)
    ]
    share = dot(
        "nkt,nkd->ntd",
        jnp.concatenate([mine[0], other[0], units_a, units_b], axis=1),
        jnp.concatenate([out_a, out_b, *spread], axis=1),
    )
    return lax.psum_scatter(
        share.astype(BF).reshape(total, width),
        "expert",
        scatter_dimension=0,
        tiled=True,
        axis_index_groups=rings,
    )


def solution(mesh):
    placed = (
        P(("groups", "expert"), "tensor"),
        P(("groups", "expert"), None),
        P(("groups", "expert"), None),
        P("tensor", "expert"),
        P("tensor", "expert"),
        P("expert", "tensor"),
        P(None, "expert", "tensor"),
        P("expert", "tensor"),
    )

    return jax.shard_map(
        local,
        mesh=mesh,
        in_specs=placed,
        out_specs=P(("groups", "expert"), "tensor"),
        check_vma=False,
    )
```

```python
import jax
import jax.numpy as jnp
from jax import lax
from jax.sharding import PartitionSpec as P


FFE = 1024
CAP = 48
CORES = 2
BF = jnp.bfloat16
F32 = jnp.float32


def dot(spec, a, b):
    return jnp.einsum(spec, a, b, preferred_element_type=F32)


def route(info, columns, top):
    tok = info.shape[2]
    own = (lax.axis_index("expert") * columns // FFE).astype(F32)
    hit = info[:, :top, :] == own
    named = jnp.any(hit, axis=1)
    weight = jnp.sum(jnp.where(hit, info[:, top:, :], 0.0), axis=1)
    order = jnp.arange(tok)
    before = (order[:, None] < order[None, :]).astype(BF)
    position = dot("ns,st->nt", named.astype(BF), before).astype(jnp.int32)
    return jnp.where(named, position, -1), weight


def local(tokens, choices, affinity, expert_gate, expert_up, expert_down, shared_in, shared_down):
    tok, width = tokens.shape
    columns = expert_gate.shape[1]
    units = shared_in.shape[1]
    top = choices.shape[1]
    blocks = lax.axis_size("expert")
    parts = lax.axis_size("tensor")
    pieces = FFE // columns
    near = blocks // pieces
    chips = parts // CORES
    half = CAP // CORES
    core = lax.axis_index("tensor") % CORES
    rings = [[r + pieces * k for k in range(near)] for r in range(pieces)]
    crosses = [[c + CORES * k for k in range(chips)] for c in range(CORES)]
    partner = [(t, t - t % CORES + (t + 1) % CORES) for t in range(parts)]

    def with_mates(array):
        moved = [
            lax.ppermute(
                array, "expert", [(z, z - z % pieces + (z + shift) % pieces) for z in range(blocks)]
            )
            for shift in range(1, pieces)
        ]
        return [array] + moved

    everyone = lax.all_gather(tokens, "expert", axis=0, tiled=True, axis_index_groups=rings)
    gates = with_mates(expert_gate)
    small = jnp.concatenate([shared_in.reshape(2 * units, width), shared_down], axis=0)
    small = with_mates(small)
    sigmoids = jax.nn.sigmoid(affinity)
    mix = 2.5 * sigmoids / jnp.sum(sigmoids, axis=1, keepdims=True)
    info = jnp.concatenate([choices.astype(F32).T, mix.T], axis=0)
    info = lax.all_to_all(
        jnp.broadcast_to(info[None], (near, *info.shape)),
        "expert",
        split_axis=0,
        concat_axis=0,
        tiled=True,
        axis_index_groups=rings,
    )
    slot, weight = route(info, columns, top)
    shared = jnp.stack([s.reshape(3, units, width) for s in small], axis=1)
    shared = shared.reshape(3, CORES, pieces * units // CORES, width)

    def side(which):
        numbers = which * half + jnp.arange(half, dtype=jnp.int32)
        picks = slot[:, None, :] == numbers[None, :, None]
        slot_weight = jnp.sum(jnp.where(picks, weight[:, None, :], 0.0), axis=2)
        rows = lax.dynamic_index_in_dim(shared, which, axis=1, keepdims=False)
        return picks.astype(BF), slot_weight, rows

    mine, other = side(core), side(1 - core)
    total = near * tok
    rows = near * half // chips
    late_up, down, everyone = lax.optimization_barrier((expert_up, expert_down, everyone))
    ups = with_mates(late_up)
    downs = jnp.concatenate(with_mates(down), axis=0)
    received = dot(
        "nct,ntd->ncd",
        jnp.concatenate([other[0], mine[0]], axis=1),
        everyone.reshape(near, tok, width),
    ).astype(BF)
    received = received.reshape(near, CORES, half, width)
    received = [received[:, 1 - c].reshape(chips, rows, width) for c in range(CORES)]
    wanted = jnp.stack([side_of[2][:2] for side_of in (mine, other)])
    wanted = wanted.reshape(CORES, 2, chips, -1, width).transpose(0, 2, 1, 3, 4)
    shared_sums = dot("hd,td->ht", wanted.reshape(-1, width), everyone).astype(BF)
    shared_sums = shared_sums.reshape(CORES, chips, -1, columns)

    def first(which):
        weights = jnp.concatenate([*gates, expert_up], axis=1)
        return dot("jrd,dp->jrp", received[which], weights).astype(BF)

    def second(which):
        late = [dot("jrd,dp->jrp", received[which], up).astype(BF) for up in ups[1:]]
        return jnp.concatenate([*late, shared_sums[which]], axis=1)

    def summed(partials):
        theirs = lax.ppermute(partials(1), "tensor", partner)
        both = (partials(0).astype(F32) + theirs.astype(F32)).astype(BF)
        crossed = lax.all_to_all(
            both, "tensor", split_axis=0, concat_axis=0, tiled=True, axis_index_groups=crosses
        )
        return jnp.sum(crossed.astype(F32), axis=0)

    early, late = summed(first), summed(second)
    gate_of, up_of = early[:, :FFE], [early[:, FFE:]]
    up_of += [late[rows * p : rows * (p + 1)] for p in range(pieces - 1)]
    pair = late[rows * (pieces - 1) :].reshape(2, -1, total)
    routed = [
        (jax.nn.silu(gate_of[:, columns * p : columns * (p + 1)]) * up_of[p]).astype(BF)
        for p in range(pieces)
    ]
    routed = jnp.concatenate(routed, axis=1)
    shared_hidden = (jax.nn.silu(pair[0]) * pair[1]).astype(BF).reshape(-1, FFE)
    hidden = jnp.concatenate([routed, shared_hidden], axis=0)
    hidden = lax.all_gather(hidden, "tensor", axis=0, axis_index_groups=crosses)
    their_hidden = lax.ppermute(hidden, "tensor", partner)

    def outs(hidden, slot_weight):
        out = dot("rp,pd->rd", hidden[:, :rows].reshape(near * half, FFE), downs)
        out = (out.reshape(near, half, width) * slot_weight[:, :, None]).astype(BF)
        units_of = hidden[:, rows:].reshape(-1, near, tok).transpose(1, 0, 2)
        return out, units_of

    (out_a, units_a), (out_b, units_b) = outs(hidden, mine[1]), outs(their_hidden, other[1])
    spread = [
        jnp.broadcast_to(s[2][2], (near, *s[2].shape[1:])) for s in (mine, other)
    ]
    share = dot(
        "nkt,nkd->ntd",
        jnp.concatenate([mine[0], other[0], units_a, units_b], axis=1),
        jnp.concatenate([out_a, out_b, *spread], axis=1),
    )
    return lax.psum_scatter(
        share.astype(BF).reshape(total, width),
        "expert",
        scatter_dimension=0,
        tiled=True,
        axis_index_groups=rings,
    )


def solution(mesh):
    placed = (
        P(("groups", "expert"), "tensor"),
        P(("groups", "expert"), None),
        P(("groups", "expert"), None),
        P("tensor", "expert"),
        P("tensor", "expert"),
        P("expert", "tensor"),
        P(None, "expert", "tensor"),
        P("expert", "tensor"),
    )

    return jax.shard_map(
        local,
        mesh=mesh,
        in_specs=placed,
        out_specs=P(("groups", "expert"), "tensor"),
        check_vma=False,
    )
```

```python
import jax
import jax.numpy as jnp
from jax import lax
from jax.sharding import PartitionSpec as P


FFE = 1024
CAP = 48
CORES = 2
BF = jnp.bfloat16
F32 = jnp.float32


def dot(spec, a, b):
    return jnp.einsum(spec, a, b, preferred_element_type=F32)


def route(info, columns, top):
    tok = info.shape[2]
    own = (lax.axis_index("expert") * columns // FFE).astype(F32)
    hit = info[:, :top, :] == own
    named = jnp.any(hit, axis=1)
    weight = jnp.sum(jnp.where(hit, info[:, top:, :], 0.0), axis=1)
    order = jnp.arange(tok)
    before = (order[:, None] < order[None, :]).astype(BF)
    position = dot("ns,st->nt", named.astype(BF), before).astype(jnp.int32)
    return jnp.where(named, position, -1), weight


def local(tokens, choices, affinity, expert_gate, expert_up, expert_down, shared_in, shared_down):
    tok, width = tokens.shape
    columns = expert_gate.shape[1]
    units = shared_in.shape[1]
    top = choices.shape[1]
    blocks = lax.axis_size("expert")
    parts = lax.axis_size("tensor")
    pieces = FFE // columns
    near = blocks // pieces
    chips = parts // CORES
    half = CAP // CORES
    core = lax.axis_index("tensor") % CORES
    rings = [[r + pieces * k for k in range(near)] for r in range(pieces)]
    crosses = [[c + CORES * k for k in range(chips)] for c in range(CORES)]
    partner = [(t, t - t % CORES + (t + 1) % CORES) for t in range(parts)]

    def with_mates(array):
        moved = [
            lax.ppermute(
                array, "expert", [(z, z - z % pieces + (z + shift) % pieces) for z in range(blocks)]
            )
            for shift in range(1, pieces)
        ]
        return [array] + moved

    everyone = lax.all_gather(tokens, "expert", axis=0, tiled=True, axis_index_groups=rings)
    gates = with_mates(expert_gate)
    small = jnp.concatenate([shared_in.reshape(2 * units, width), shared_down], axis=0)
    small = with_mates(small)
    sigmoids = jax.nn.sigmoid(affinity)
    mix = 2.5 * sigmoids / jnp.sum(sigmoids, axis=1, keepdims=True)
    info = jnp.concatenate([choices.astype(F32).T, mix.T], axis=0)
    info = lax.all_to_all(
        jnp.broadcast_to(info[None], (near, *info.shape)),
        "expert",
        split_axis=0,
        concat_axis=0,
        tiled=True,
        axis_index_groups=rings,
    )
    slot, weight = route(info, columns, top)
    shared = jnp.stack([s.reshape(3, units, width) for s in small], axis=1)
    shared = shared.reshape(3, CORES, pieces * units // CORES, width)

    def side(which):
        numbers = which * half + jnp.arange(half, dtype=jnp.int32)
        picks = slot[:, None, :] == numbers[None, :, None]
        slot_weight = jnp.sum(jnp.where(picks, weight[:, None, :], 0.0), axis=2)
        rows = lax.dynamic_index_in_dim(shared, which, axis=1, keepdims=False)
        return picks.astype(BF), slot_weight, rows

    mine, other = side(core), side(1 - core)
    total = near * tok
    rows = near * half // chips
    late_up, down, everyone = lax.optimization_barrier((expert_up, expert_down, everyone))
    ups = with_mates(late_up)
    downs = jnp.concatenate(with_mates(down), axis=0)
    received = dot(
        "nct,ntd->ncd",
        jnp.concatenate([other[0], mine[0]], axis=1),
        everyone.reshape(near, tok, width),
    ).astype(BF)
    received = received.reshape(near, CORES, half, width)
    received = [received[:, 1 - c].reshape(chips, rows, width) for c in range(CORES)]
    wanted = jnp.stack([side_of[2][:2] for side_of in (mine, other)])
    wanted = wanted.reshape(CORES, 2, chips, -1, width).transpose(0, 2, 1, 3, 4)
    shared_sums = dot("hd,td->ht", wanted.reshape(-1, width), everyone).astype(BF)
    shared_sums = shared_sums.reshape(CORES, chips, -1, FFE)

    def first(which):
        return dot("jrd,dp->jrp", received[which], jnp.concatenate(gates, axis=1)).astype(BF)

    def second(which):
        late = dot("jrd,dp->jrp", received[which], jnp.concatenate(ups, axis=1)).astype(BF)
        return jnp.concatenate([late, shared_sums[which]], axis=1)

    def summed(partials):
        theirs = lax.ppermute(partials(1), "tensor", partner)
        both = (partials(0).astype(F32) + theirs.astype(F32)).astype(BF)
        crossed = lax.all_to_all(
            both, "tensor", split_axis=0, concat_axis=0, tiled=True, axis_index_groups=crosses
        )
        return jnp.sum(crossed.astype(F32), axis=0)

    early, late = summed(first), summed(second)
    routed = (jax.nn.silu(early) * late[:rows]).astype(BF)
    pair = late[rows:].reshape(2, -1, total)
    shared_hidden = (jax.nn.silu(pair[0]) * pair[1]).astype(BF).reshape(-1, FFE)
    hidden = jnp.concatenate([routed, shared_hidden], axis=0)
    hidden = lax.all_gather(hidden, "tensor", axis=0, axis_index_groups=crosses)
    their_hidden = lax.ppermute(hidden, "tensor", partner)

    def outs(hidden, slot_weight):
        out = dot("rp,pd->rd", hidden[:, :rows].reshape(near * half, FFE), downs)
        out = (out.reshape(near, half, width) * slot_weight[:, :, None]).astype(BF)
        units_of = hidden[:, rows:].reshape(-1, near, tok).transpose(1, 0, 2)
        return out, units_of

    (out_a, units_a), (out_b, units_b) = outs(hidden, mine[1]), outs(their_hidden, other[1])
    spread = [
        jnp.broadcast_to(s[2][2], (near, *s[2].shape[1:])) for s in (mine, other)
    ]
    share = dot(
        "nkt,nkd->ntd",
        jnp.concatenate([mine[0], other[0], units_a, units_b], axis=1),
        jnp.concatenate([out_a, out_b, *spread], axis=1),
    )
    return lax.psum_scatter(
        share.astype(BF).reshape(total, width),
        "expert",
        scatter_dimension=0,
        tiled=True,
        axis_index_groups=rings,
    )


def solution(mesh):
    placed = (
        P(("groups", "expert"), "tensor"),
        P(("groups", "expert"), None),
        P(("groups", "expert"), None),
        P("tensor", "expert"),
        P("tensor", "expert"),
        P("expert", "tensor"),
        P(None, "expert", "tensor"),
        P("expert", "tensor"),
    )

    return jax.shard_map(
        local,
        mesh=mesh,
        in_specs=placed,
        out_specs=P(("groups", "expert"), "tensor"),
        check_vma=False,
    )
```
